32 devices in a mesh: seq: 4 (over x, core), fsdp: 8 (over z, y).
Axes of the slice: x: 2, y: 2, z: 4, core: 2. Of those that a mesh axis runs over, the one named last changes fastest.
Arguments:
- tokens: bfloat16 [8, 1024, 2048], P('fsdp', 'seq'), may hold values from -6 to 6
- targets: bfloat16 [8, 1024, 2048], P('fsdp', 'seq'), may hold values from -6 to 6
- lengths: int32 [8], replicated, may hold values from 1 to 1024, 6144 in all
- w_qkv: float32 [2048, 3, 2048], P('fsdp', None, 'seq'), may hold values from -0.125 to 0.125
- w_out: float32 [2048, 2048], P('seq', 'fsdp'), may hold values from -1 to 1
- w_gateup: float32 [2048, 2, 8192], P('fsdp', None, 'seq'), may hold values from -0.125 to 0.125
- w_down: float32 [8192, 2048], P('seq', 'fsdp'), may hold values from -0.0625 to 0.0625
- mom_qkv: float32 [2048, 3, 2048], P('fsdp', None, 'seq'), may hold values from -0.0390625 to 0.0390625
- mom_out: float32 [2048, 2048], P('seq', 'fsdp'), may hold values from -0.0234375 to 0.0234375
- mom_gateup: float32 [2048, 2, 8192], P('fsdp', None, 'seq'), may hold values from -0.0390625 to 0.0390625
- mom_down: float32 [8192, 2048], P('seq', 'fsdp'), may hold values from -0.078125 to 0.078125
- avg_qkv: float32 [2048, 3, 2048], P('fsdp', None, 'seq'), may hold values from -0.125 to 0.125
- avg_out: float32 [2048, 2048], P('seq', 'fsdp'), may hold values from -1 to 1
- avg_gateup: float32 [2048, 2, 8192], P('fsdp', None, 'seq'), may hold values from -0.125 to 0.125
- avg_down: float32 [8192, 2048], P('seq', 'fsdp'), may hold values from -0.0625 to 0.0625
Outputs:
- output: bfloat16 [8, 1024, 2048], P('fsdp', 'seq')
- input_grad: bfloat16 [8, 1024, 2048], P('fsdp', 'seq')
- loss: float32 [], replicated
- new_qkv: float32 [2048, 3, 2048], P('fsdp', None, 'seq')
- new_out: float32 [2048, 2048], P('seq', 'fsdp')
- new_gateup: float32 [2048, 2, 8192], P('fsdp', None, 'seq')
- new_down: float32 [8192, 2048], P('seq', 'fsdp')
- newmom_qkv: float32 [2048, 3, 2048], P('fsdp', None, 'seq')
- newmom_out: float32 [2048, 2048], P('seq', 'fsdp')
- newmom_gateup: float32 [2048, 2, 8192], P('fsdp', None, 'seq')
- newmom_down: float32 [8192, 2048], P('seq', 'fsdp')
- newavg_qkv: float32 [2048, 3, 2048], P('fsdp', None, 'seq')
- newavg_out: float32 [2048, 2048], P('seq', 'fsdp')
- newavg_gateup: float32 [2048, 2, 8192], P('fsdp', None, 'seq')
- newavg_down: float32 [8192, 2048], P('seq', 'fsdp')
The draws below stay inside these ranges and needn't reach their ends.
Inputs may be any that keep to these rules, and one draw needn't show every extreme that they name: lengths[s] valid tokens stand first in sequence s's 1024 slots, padding after; they sum to 6144 and one equals 1024.
All inputs are finite; a program needn't handle non-finite values.
Results may differ from the reference program's by a relative error of at most 0.015.
Values may be sent and summed in bfloat16 or wider, within the bound.
A program may use at most 256 MiB of HBM per device.

```python
import math
import jax
import jax.numpy as jnp
import numpy as np
from jax import lax

D = 2048
HEADS = 16
HD = 128
FF = 8192
SEQ_LEN = 1024
SEQS = 8
SLOTS = 8192


def block_scale(key, shape, cuts, smallest, high):
    loudness = 1.0
    for dim, parts in cuts:
        steps = jax.random.uniform(jax.random.fold_in(jax.random.fold_in(key, 6), dim), (parts,), jnp.float32, smallest / len(cuts), high / len(cuts))
        loudness = loudness * jnp.repeat(jnp.exp(steps), shape[dim] // parts).reshape((-1,) + (1,) * (len(shape) - 1 - dim))
    return loudness


def profile(amount, total, most, skew):
    loads = [(1 << 20) // math.isqrt(grade ** skew) + 1 for grade in range(2, amount + 1)]
    rest, given = total - most - (amount - 1), [1] * (amount - 1)
    while rest > 0:
        candidates = [i for i in range(amount - 1) if given[i] < most]
        whole, budget = sum([loads[i] for i in candidates]), rest
        for i in candidates:
            addition = min(most - given[i], max(1, budget * loads[i] // whole), rest)
            given[i] = given[i] + addition
            rest = rest - addition
    return np.array([most] + given)


def uneven(stream_key, number_of, total, limit, skew):
    if number_of == 2:
        one = jax.random.randint(stream_key, (), max(1, total - limit), min(limit, total - 1) + 1)
        return jnp.stack([one, total - one])
    sizes = jnp.asarray(profile(number_of, total, limit, skew), jnp.int32)
    twos = (number_of - 1) // 2
    giver, taker = sizes[1:1 + 2 * twos:2], sizes[2:2 + 2 * twos:2]
    slack = jnp.minimum(giver - 1, limit - taker)
    moved = jax.random.randint(jax.random.fold_in(stream_key, 1), (twos,), 0, 1 << 20) % (slack + 1)
    sizes = sizes.at[1:1 + 2 * twos:2].set(giver - moved).at[2:2 + 2 * twos:2].set(taker + moved)
    return sizes[jax.random.permutation(jax.random.fold_in(stream_key, 2), number_of)]


def normal_values(stream_key, extent, width, reach, split=(), held_as=jnp.bfloat16):
    factor_of = block_scale(stream_key, extent, split, -0.22, 0.18) if split else 1.0
    array = jax.random.normal(stream_key, extent, jnp.float32) * width * factor_of
    return jnp.minimum(jnp.maximum(array, -reach), reach).astype(held_as)


def setup_inputs(seed: int = 0) -> dict:
    key_of = jax.random.split(jax.random.key(seed), 16)
    tokens = normal_values(key_of[0], (SEQS, SEQ_LEN, D), 1.0, 6.0, ((0, 8), (1, 4)))
    targets = normal_values(key_of[1], (SEQS, SEQ_LEN, D), 1.0, 6.0, ((0, 8), (1, 4)))
    lengths = uneven(key_of[2], SEQS, 3 * SEQS * SEQ_LEN // 4, SEQ_LEN, 1).astype(jnp.int32)
    w_qkv = normal_values(key_of[3], (D, 3, D), D ** -0.5, 0.125, ((0, 8), (2, 4)), jnp.float32)
    w_out = normal_values(key_of[4], (D, D), (D // 64) ** -0.5, 1.0, ((0, 4), (1, 8)), jnp.float32)
    w_gateup = normal_values(key_of[5], (D, 2, FF), D ** -0.5, 0.125, ((0, 8), (2, 4)), jnp.float32)
    w_down = normal_values(key_of[6], (FF, D), FF ** -0.5, 0.0625, ((0, 4), (1, 8)), jnp.float32)
    mom_qkv = normal_values(key_of[7], (D, 3, D), (0.5 * (3 * SLOTS // 4) ** -0.5), 0.0390625, ((0, 8), (2, 4)), jnp.float32)
    mom_out = normal_values(key_of[8], (D, D), (0.3 * (3 * SLOTS // 4) ** -0.5), 0.0234375, ((0, 4), (1, 8)), jnp.float32)
    mom_gateup = normal_values(key_of[9], (D, 2, FF), (0.5 * (3 * SLOTS // 4) ** -0.5), 0.0390625, ((0, 8), (2, 4)), jnp.float32)
    mom_down = normal_values(key_of[10], (FF, D), (1.0 * (3 * SLOTS // 4) ** -0.5), 0.078125, ((0, 4), (1, 8)), jnp.float32)
    avg_qkv = normal_values(key_of[11], (D, 3, D), D ** -0.5, 0.125, ((0, 8), (2, 4)), jnp.float32)
    avg_out = normal_values(key_of[12], (D, D), (D // 64) ** -0.5, 1.0, ((0, 4), (1, 8)), jnp.float32)
    avg_gateup = normal_values(key_of[13], (D, 2, FF), D ** -0.5, 0.125, ((0, 8), (2, 4)), jnp.float32)
    avg_down = normal_values(key_of[14], (FF, D), FF ** -0.5, 0.0625, ((0, 4), (1, 8)), jnp.float32)
    return dict(tokens=tokens, targets=targets, lengths=lengths, w_qkv=w_qkv, w_out=w_out, w_gateup=w_gateup, w_down=w_down, mom_qkv=mom_qkv, mom_out=mom_out, mom_gateup=mom_gateup, mom_down=mom_down, avg_qkv=avg_qkv, avg_out=avg_out, avg_gateup=avg_gateup, avg_down=avg_down)


EPS = 1e-05
ROPE_BASE = 10000.0
MOMENT = 0.9
KEEP = 0.95
NEG = -1e+30
HIGHEST = lax.Precision.HIGHEST

@jax.custom_vjp
def low(v):
    return lax.optimization_barrier(v.astype(jnp.bfloat16)).astype(jnp.float32)

@jax.custom_vjp
def low_back(v):
    return v

def low_keep(v):
    return (low(v), None)

def low_pass(kept, grad):
    return (grad,)

def back_keep(v):
    return (v, None)

def back_low(kept, grad):
    return (low(grad),)
low.defvjp(low_keep, low_pass)
low_back.defvjp(back_keep, back_low)

def layer_norm(values):
    centred = values - lax.optimization_barrier(jnp.mean(values, axis=-1, keepdims=True))
    return centred * lax.rsqrt(lax.optimization_barrier(jnp.mean(centred * centred, axis=-1, keepdims=True)) + EPS)

def rotary(span):
    half = HD // 2
    freq = ROPE_BASE ** (-2.0 * jnp.arange(half, dtype=jnp.float32) / HD)
    angle = jnp.arange(span, dtype=jnp.float32)[:, None] * freq[None, :]
    cosine = jnp.concatenate([jnp.cos(angle), jnp.cos(angle)], axis=-1)[:, None, :]
    sine = jnp.concatenate([jnp.sin(angle), jnp.sin(angle)], axis=-1)[:, None, :]
    return (cosine, sine)

def rotate(values):
    half = values.shape[-1] // 2
    return jnp.concatenate([-values[..., half:], values[..., :half]], axis=-1)

def attend(queries, keys_rot, values_v, length):
    span = queries.shape[0]
    block_rows = min(512, span)
    positions = jnp.arange(span, dtype=jnp.int32)
    scale = HD ** (-0.5)

    def one_block(first_row):
        rows_q = lax.dynamic_slice_in_dim(queries, first_row, block_rows, 0)
        scores = low_back(jnp.einsum('qhd,khd->hqk', rows_q, keys_rot, precision=HIGHEST) * scale)
        query_pos = first_row + jnp.arange(block_rows, dtype=jnp.int32)
        allowed = (positions[None, :] <= query_pos[:, None]) & (positions[None, :] < length)
        scores = jnp.where(allowed[None], scores, NEG)
        attn_probs = jax.nn.softmax(scores, axis=-1)
        return jnp.einsum('hqk,khd->qhd', low(attn_probs), values_v, precision=HIGHEST)
    starts = (jnp.arange(span // block_rows) * block_rows).astype(jnp.int32)
    outs = lax.map(jax.checkpoint(one_block), starts)
    return outs.reshape(span, queries.shape[1], queries.shape[2])

def forward(inputs, target, length, count, w_qkv, w_out, w_gateup, w_down):
    span = inputs.shape[0]
    normed_one = low(layer_norm(inputs))
    qkv_all = low_back(jnp.einsum('td,djc->tjc', normed_one, low(w_qkv), precision=HIGHEST))
    cosine, sine = rotary(span)
    queries = qkv_all[:, 0].reshape(span, HEADS, HD)
    keys_rot = qkv_all[:, 1].reshape(span, HEADS, HD)
    queries = low(queries * cosine + rotate(queries) * sine)
    keys_rot = low(keys_rot * cosine + rotate(keys_rot) * sine)
    values_v = low(qkv_all[:, 2].reshape(span, HEADS, HD))
    attended = low_back(low(attend(queries, keys_rot, values_v, length).reshape(span, D)))
    middle = inputs + low_back(jnp.dot(attended, low(w_out), precision=HIGHEST))
    normed_two = low(layer_norm(middle))
    gate_up = low_back(jnp.einsum('td,djf->tjf', normed_two, low(w_gateup), precision=HIGHEST))
    hidden = low(jax.nn.silu(gate_up[:, 0]) * gate_up[:, 1])
    result = middle + low_back(jnp.dot(hidden, low(w_down), precision=HIGHEST))
    valid = (jnp.arange(span, dtype=jnp.int32) < length)[:, None]
    diff = jnp.where(valid, result - target, 0.0)
    return (jnp.sum(diff * diff) / (2.0 * count), result)

def advance(weight, moment, average, grad, rate):
    moment_new = MOMENT * moment + grad
    weight_new = weight - rate * (grad + MOMENT * moment_new)
    average_new = KEEP * average + (1.0 - KEEP) * weight_new
    return (weight_new, moment_new, average_new)

def reference(tokens, targets, lengths, w_qkv, w_out, w_gateup, w_down, mom_qkv, mom_out, mom_gateup, mom_down, avg_qkv, avg_out, avg_gateup, avg_down):
    count = jnp.sum(lengths).astype(jnp.float32)

    def per_sequence(carry, item):
        seq_tokens, seq_target, length = item

        def local(inputs, weight_a, weight_b, weight_c, weight_d):
            return forward(inputs, seq_target, length, count, weight_a, weight_b, weight_c, weight_d)
        (loss_part, result), pull = jax.vjp(local, seq_tokens.astype(jnp.float32), w_qkv, w_out, w_gateup, w_down)
        grads = pull((jnp.ones_like(loss_part), jnp.zeros_like(result)))
        carry = (carry[0] + loss_part, carry[1] + grads[1], carry[2] + grads[2], carry[3] + grads[3], carry[4] + grads[4])
        return (carry, (result.astype(jnp.bfloat16), grads[0].astype(jnp.bfloat16)))
    init = (jnp.zeros((), jnp.float32), jnp.zeros_like(w_qkv), jnp.zeros_like(w_out), jnp.zeros_like(w_gateup), jnp.zeros_like(w_down))
    totals, (output, input_grad) = lax.scan(per_sequence, init, (tokens, targets.astype(jnp.float32), lengths))
    loss, grad_qkv, grad_out, grad_gateup, grad_down = totals
    new_qkv, newmom_qkv, newavg_qkv = advance(w_qkv, mom_qkv, avg_qkv, grad_qkv, 2.0)
    new_out, newmom_out, newavg_out = advance(w_out, mom_out, avg_out, grad_out, 20.0)
    new_gateup, newmom_gateup, newavg_gateup = advance(w_gateup, mom_gateup, avg_gateup, grad_gateup, 2.0)
    new_down, newmom_down, newavg_down = advance(w_down, mom_down, avg_down, grad_down, 1.0)
    return (output, input_grad, loss, new_qkv, new_out, new_gateup, new_down, newmom_qkv, newmom_out, newmom_gateup, newmom_down, newavg_qkv, newavg_out, newavg_gateup, newavg_down)
```

```python
import jax
import jax.numpy as jnp
from jax import lax
from jax.sharding import PartitionSpec as P

HD = 128


EPS = 1e-05
ROPE_BASE = 10000.0
MOMENT = 0.9
KEEP = 0.95
NEG = -1e30


def layer_norm(values):
    centred = values - jnp.mean(values, axis=-1, keepdims=True)
    factor = lax.rsqrt(jnp.mean(centred * centred, axis=-1, keepdims=True) + EPS)
    return (centred * factor, factor)


def norm_back(grad, normed, factor):
    inner = jnp.mean(grad * normed, axis=-1, keepdims=True)
    return factor * (grad - jnp.mean(grad, axis=-1, keepdims=True) - normed * inner)


def rotary(positions, width):
    half = width // 2
    freq = ROPE_BASE ** (-2.0 * jnp.arange(half, dtype=jnp.float32) / width)
    angle = positions.astype(jnp.float32)[:, None] * freq[None, :]
    cosine = jnp.concatenate([jnp.cos(angle), jnp.cos(angle)], axis=-1)[:, None, :]
    sine = jnp.concatenate([jnp.sin(angle), jnp.sin(angle)], axis=-1)[:, None, :]
    return (cosine, sine)


def rotate(values):
    half = values.shape[-1] // 2
    return jnp.concatenate([-values[..., half:], values[..., :half]], axis=-1)


def unrotate(values):
    half = values.shape[-1] // 2
    return jnp.concatenate([values[..., half:], -values[..., :half]], axis=-1)


def allowed_mask(first_row, block_rows, positions, length):
    query_pos = lax.dynamic_slice_in_dim(positions, first_row, block_rows, 0)
    return (positions[None, :] <= query_pos[:, None]) & (positions[None, :] < length)


def attend_forward(queries, keys_rot, values_v, positions, length):
    span = queries.shape[0]
    block_rows = min(512, span)
    scale = queries.shape[2] ** (-0.5)

    def one_block(first_row):
        rows_q = lax.dynamic_slice_in_dim(queries, first_row, block_rows, 0)
        scores = (
            jnp.einsum("qhd,khd->hqk", rows_q, keys_rot, preferred_element_type=jnp.float32) * scale
        )
        scores = jnp.where(allowed_mask(first_row, block_rows, positions, length)[None], scores, NEG)
        highest = jnp.max(scores, axis=-1, keepdims=True)
        expvals = jnp.exp(scores - highest)
        totals = jnp.sum(expvals, axis=-1, keepdims=True)
        attn_probs = (expvals / totals).astype(jnp.bfloat16)
        outs = jnp.einsum("hqk,khd->qhd", attn_probs, values_v, preferred_element_type=jnp.float32)
        return (outs, highest[..., 0] + jnp.log(totals[..., 0]))

    starts = jnp.arange(span // block_rows) * block_rows
    outs, log_totals = lax.map(one_block, starts)
    return (outs.reshape(span, queries.shape[1], queries.shape[2]), log_totals)


def attend_back(queries, keys_rot, values_v, grad_out, log_totals, positions, length):
    span = queries.shape[0]
    block_rows = min(512, span)
    scale = queries.shape[2] ** (-0.5)
    starts = jnp.arange(span // block_rows) * block_rows

    def one_block(carry, item):
        first_row, lse_block = item
        rows_q = lax.dynamic_slice_in_dim(queries, first_row, block_rows, 0)
        rows_g = lax.dynamic_slice_in_dim(grad_out, first_row, block_rows, 0)
        scores = (
            jnp.einsum("qhd,khd->hqk", rows_q, keys_rot, preferred_element_type=jnp.float32) * scale
        )
        allowed = allowed_mask(first_row, block_rows, positions, length)[None]
        attn_probs = jnp.where(allowed, jnp.exp(scores - lse_block[..., None]), 0.0)
        probs_low = attn_probs.astype(jnp.bfloat16)
        grad_values = carry[1] + jnp.einsum(
            "hqk,qhd->khd", probs_low, rows_g, preferred_element_type=jnp.float32
        )
        grad_probs = jnp.einsum(
            "qhd,khd->hqk", rows_g, values_v, preferred_element_type=jnp.float32
        )
        inner = jnp.sum(attn_probs * grad_probs, axis=-1, keepdims=True)
        grad_scores = (attn_probs * (grad_probs - inner)).astype(jnp.bfloat16)
        grad_rows = (
            jnp.einsum("hqk,khd->qhd", grad_scores, keys_rot, preferred_element_type=jnp.float32)
            * scale
        )
        grad_keys = (
            carry[0]
            + jnp.einsum("hqk,qhd->khd", grad_scores, rows_q, preferred_element_type=jnp.float32)
            * scale
        )
        return ((grad_keys, grad_values), grad_rows)

    zeros_kv = jnp.zeros(keys_rot.shape, jnp.float32)
    (grad_keys, grad_values), grad_rows = lax.scan(
        one_block, (zeros_kv, zeros_kv), (starts, log_totals)
    )
    return (grad_rows.reshape(queries.shape), grad_keys, grad_values)


def advance(weight, moment, average, grad, rate):
    moment_new = MOMENT * moment + grad
    weight_new = weight - rate * (grad + MOMENT * moment_new)
    average_new = KEEP * average + (1.0 - KEEP) * weight_new
    return (weight_new, moment_new, average_new)


def flip(size, bit):
    return [(i, i ^ bit) for i in range(size)]


def ring(size):
    return [(i, (i + 2) % size) for i in range(size)]


def send(value, axis, pairs):
    return lax.ppermute(value, axis, pairs)


def gather_far_first(shard, members):
    blocks = [shard]
    for _ in range(members // 2 - 1):
        blocks.append(send(blocks[-1], "fsdp", ring(members)))
    return blocks + [send(block, "fsdp", flip(members, 1)) for block in blocks]


def gather_near_first(shard, members):
    blocks = []
    for start in (shard, send(shard, "fsdp", flip(members, 1))):
        blocks.append(start)
        for _ in range(members // 2 - 1):
            blocks.append(send(blocks[-1], "fsdp", ring(members)))
    return blocks


def add_low(one, two):
    return (one.astype(jnp.float32) + two.astype(jnp.float32)).astype(jnp.bfloat16)


def ring_sum(blocks, members):
    depth = len(blocks)
    moving = blocks[1]
    for j in range(2, depth + 1):
        moving = send(moving, "fsdp", ring(members))
        if j < depth:
            moving = add_low(moving, blocks[j])
    return blocks[0].astype(jnp.float32) + moving.astype(jnp.float32)


def scatter_near_first(blocks, members):
    depth = members // 2
    order = list(range(1, depth)) + [0]
    kept = [None] * depth
    for j in order:
        kept[j] = add_low(blocks[j], send(blocks[depth + j], "fsdp", flip(members, 1)))
    return ring_sum(kept, members)


def scatter_far_first(blocks, members):
    depth = members // 2
    other = ring_sum(blocks[depth:], members).astype(jnp.bfloat16)
    mine = ring_sum(blocks[:depth], members)
    return mine + send(other, "fsdp", flip(members, 1)).astype(jnp.float32)


def gather_group(block, size):
    blocks = [block]
    bit = size // 2
    while bit:
        blocks = blocks + [send(b, "seq", flip(size, bit)) for b in blocks]
        bit //= 2
    order = [0] * size
    place = [0]
    bit = size // 2
    while bit:
        place = place + [p ^ bit for p in place]
        bit //= 2
    for at, p in enumerate(place):
        order[p] = at
    return jnp.concatenate([blocks[at] for at in order], axis=0)


def scatter_group(values, size):
    rows = values.shape[0] // size
    blocks = {r: values[r * rows:(r + 1) * rows] for r in range(size)}
    bit = 1
    while bit < size:
        kept = {}
        for r in blocks:
            if not r & bit:
                arrived = send(blocks[r ^ bit], "seq", flip(size, bit))
                kept[r] = blocks[r].astype(jnp.float32) + arrived.astype(jnp.float32)
        bit *= 2
        blocks = kept if bit == size else {r: v.astype(jnp.bfloat16) for r, v in kept.items()}
    return blocks[0]


def total_of(value, size_seq, size_fsdp):
    for axis, size in (("seq", size_seq), ("fsdp", size_fsdp)):
        bit = 1
        while bit < size:
            value = value + send(value, axis, flip(size, bit))
            bit *= 2
    return value


def reorder(values, member, members):
    width = values.shape[-1] // members
    depth = members // 2
    outer, inner = member // 2, member % 2
    return outer, inner, width, depth


def to_ring(values, member, members):
    outer, inner, width, depth = reorder(values, member, members)
    parts = []
    for i in range(2):
        for j in range(depth):
            block = lax.rem(outer - j + depth, depth) * 2 + (inner ^ i)
            parts.append(lax.dynamic_slice_in_dim(values, block * width, width, 1))
    return jnp.concatenate(parts, axis=1)


def from_ring(values, member, members):
    outer, inner, width, depth = reorder(values, member, members)
    parts = []
    for block in range(members):
        at = (inner ^ (block % 2)) * depth + lax.rem(outer - block // 2 + depth, depth)
        parts.append(lax.dynamic_slice_in_dim(values, at * width, width, 1))
    return jnp.concatenate(parts, axis=1)


def split_rows(values, members):
    rows = values.shape[0] // members
    return [values[p * rows:(p + 1) * rows] for p in range(members)]


def split_cols(values, members):
    cols = values.shape[1] // members
    return [values[:, p * cols:(p + 1) * cols] for p in range(members)]

def on_device(
    tokens,
    targets,
    lengths,
    w_qkv,
    w_out,
    w_gateup,
    w_down,
    mom_qkv,
    mom_out,
    mom_gateup,
    mom_down,
    avg_qkv,
    avg_out,
    avg_gateup,
    avg_down,
):
    n_shards = lax.axis_size("seq")
    members = lax.axis_size("fsdp")
    shard_index = lax.axis_index("seq")
    member = lax.axis_index("fsdp")
    own_rows = tokens.shape[1]
    span = own_rows * n_shards
    head_size = HD
    d_rows = w_qkv.shape[0]
    width = w_qkv.shape[2]
    ff = w_gateup.shape[2]
    heads_here = width // head_size
    low = jnp.bfloat16
    wide = jnp.float32

    inputs = to_ring(tokens[0], member, members).astype(wide)
    target = to_ring(targets[0], member, members).astype(wide)
    own_length = lax.dynamic_index_in_dim(lengths, member, 0, keepdims=False)
    count = jnp.sum(lengths).astype(wide)
    row_in_block = jnp.arange(own_rows, dtype=jnp.int32)
    positions = jnp.concatenate(
        [(shard_index ^ r) * own_rows + row_in_block for r in range(n_shards)]
    )
    own_pos = shard_index * own_rows + row_in_block
    valid = (own_pos < own_length).astype(wide)[:, None]

    blocks_qkv = gather_far_first(w_qkv.astype(low).reshape(d_rows, 3 * width), members)
    blocks_out = gather_far_first(w_out.astype(low), members)
    blocks_gateup = gather_far_first(w_gateup.astype(low).reshape(d_rows, 2 * ff), members)
    blocks_down = gather_near_first(w_down.astype(low), members)
    full_qkv = jnp.concatenate(blocks_qkv, axis=0)
    full_out = jnp.concatenate(blocks_out, axis=1)
    full_gateup = jnp.concatenate(blocks_gateup, axis=0)
    full_down = jnp.concatenate(blocks_down, axis=1)

    normed_one, factor_one = layer_norm(inputs)
    group_one = gather_group(normed_one.astype(low), n_shards)
    qkv_all = jnp.dot(group_one, full_qkv, preferred_element_type=wide)
    cosine, sine = rotary(positions, head_size)
    queries = qkv_all[:, :width].reshape(span, heads_here, head_size)
    keys_pre = qkv_all[:, width:2 * width].reshape(span, heads_here, head_size)
    queries = (queries * cosine + rotate(queries) * sine).astype(low)
    keys_rot = (keys_pre * cosine + rotate(keys_pre) * sine).astype(low)
    values_v = qkv_all[:, 2 * width:].reshape(span, heads_here, head_size).astype(low)
    attended, log_totals = attend_forward(queries, keys_rot, values_v, positions, own_length)
    attended = attended.reshape(span, width).astype(low)
    attn_term = jnp.dot(attended, full_out, preferred_element_type=wide)
    middle = inputs + scatter_group(attn_term.astype(low), n_shards)
    normed_two, factor_two = layer_norm(middle)
    group_two = gather_group(normed_two.astype(low), n_shards)
    gate_up = jnp.dot(group_two, full_gateup, preferred_element_type=wide)
    gate = gate_up[:, :ff]
    up_part = gate_up[:, ff:]
    hidden = (jax.nn.silu(gate) * up_part).astype(low)
    ffn_term = jnp.dot(hidden, full_down, preferred_element_type=wide)
    result = middle + scatter_group(ffn_term.astype(low), n_shards)
    diff = (result - target) * valid
    partial = jnp.broadcast_to(jnp.sum(diff * diff), (8, 128))
    loss = total_of(partial, n_shards, members)[0, 0] / (2.0 * count)
    grad_result = diff / count

    contract_rows = (((0,), (0,)), ((), ()))
    contract_cols = (((1,), (1,)), ((), ()))
    group_dy = gather_group(grad_result.astype(low), n_shards)
    grad_down = lax.dot_general(hidden, group_dy, contract_rows, preferred_element_type=wide)
    summed_down = scatter_far_first(split_cols(grad_down.astype(low), members), members)
    grad_hidden = lax.dot_general(
        group_dy, full_down, contract_cols, preferred_element_type=wide
    )
    sigma = jax.nn.sigmoid(gate)
    grad_gate = grad_hidden * up_part * sigma * (1.0 + gate * (1.0 - sigma))
    grad_up = grad_hidden * gate * sigma
    grad_gu = jnp.concatenate([grad_gate, grad_up], axis=1).astype(low)
    normed_grad_two = lax.dot_general(
        grad_gu, full_gateup, contract_cols, preferred_element_type=wide
    )
    grad_gateup = lax.dot_general(
        group_two, grad_gu, contract_rows, preferred_element_type=wide
    )
    summed_gateup = scatter_near_first(split_rows(grad_gateup.astype(low), members), members)
    own_grad_two = scatter_group(normed_grad_two.astype(low), n_shards)
    grad_middle = grad_result + norm_back(own_grad_two, normed_two, factor_two)
    group_da = gather_group(grad_middle.astype(low), n_shards)
    grad_att = lax.dot_general(group_da, full_out, contract_cols, preferred_element_type=wide)
    grad_att = grad_att.astype(low).reshape(span, heads_here, head_size)
    grad_out = lax.dot_general(attended, group_da, contract_rows, preferred_element_type=wide)
    summed_out = scatter_near_first(split_cols(grad_out.astype(low), members), members)
    grad_rows, grad_keys, grad_values = attend_back(
        queries, keys_rot, values_v, grad_att, log_totals, positions, own_length
    )
    grad_rows = grad_rows * cosine + unrotate(grad_rows * sine)
    grad_keys = grad_keys * cosine + unrotate(grad_keys * sine)
    grad_qkv_all = jnp.concatenate(
        [grad_rows.reshape(span, -1), grad_keys.reshape(span, -1), grad_values.reshape(span, -1)],
        axis=1,
    ).astype(low)
    grad_qkv = lax.dot_general(
        group_one, grad_qkv_all, contract_rows, preferred_element_type=wide
    )
    summed_qkv = scatter_near_first(split_rows(grad_qkv.astype(low), members), members)
    normed_grad_one = lax.dot_general(
        grad_qkv_all, full_qkv, contract_cols, preferred_element_type=wide
    )
    own_grad_one = scatter_group(normed_grad_one.astype(low), n_shards)
    grad_inputs = grad_middle + norm_back(own_grad_one, normed_one, factor_one)
    summed_qkv = summed_qkv.reshape(w_qkv.shape)
    summed_gateup = summed_gateup.reshape(w_gateup.shape)
    new_qkv, newmom_qkv, newavg_qkv = advance(w_qkv, mom_qkv, avg_qkv, summed_qkv, 2.0)
    new_out, newmom_out, newavg_out = advance(w_out, mom_out, avg_out, summed_out, 20.0)
    new_gateup, newmom_gateup, newavg_gateup = advance(
        w_gateup, mom_gateup, avg_gateup, summed_gateup, 2.0
    )
    new_down, newmom_down, newavg_down = advance(w_down, mom_down, avg_down, summed_down, 1.0)
    return (
        from_ring(result.astype(low), member, members)[None],
        from_ring(grad_inputs.astype(low), member, members)[None],
        loss,
        new_qkv,
        new_out,
        new_gateup,
        new_down,
        newmom_qkv,
        newmom_out,
        newmom_gateup,
        newmom_down,
        newavg_qkv,
        newavg_out,
        newavg_gateup,
        newavg_down,
    )


def solution(mesh):
    placed = (
        P("fsdp", "seq", None),
        P("fsdp", "seq", None),
        P(),
        P("fsdp", None, "seq"),
        P("seq", "fsdp"),
        P("fsdp", None, "seq"),
        P("seq", "fsdp"),
        P("fsdp", None, "seq"),
        P("seq", "fsdp"),
        P("fsdp", None, "seq"),
        P("seq", "fsdp"),
        P("fsdp", None, "seq"),
        P("seq", "fsdp"),
        P("fsdp", None, "seq"),
        P("seq", "fsdp"),
    )
    return jax.shard_map(
        on_device,
        mesh=mesh,
        in_specs=placed,
        out_specs=(
            P("fsdp", "seq", None),
            P("fsdp", "seq", None),
            P(),
            P("fsdp", None, "seq"),
            P("seq", "fsdp"),
            P("fsdp", None, "seq"),
            P("seq", "fsdp"),
            P("fsdp", None, "seq"),
            P("seq", "fsdp"),
            P("fsdp", None, "seq"),
            P("seq", "fsdp"),
            P("fsdp", None, "seq"),
            P("seq", "fsdp"),
            P("fsdp", None, "seq"),
            P("seq", "fsdp"),
        ),
        check_vma=False,
    )
```
